128 devices in a mesh: fsdp: 8 (over z_lo, x), tp: 16 (over y, z_hi, core).
Axes of the slice: x: 4, y: 4, z: 4 (z_hi: 2, z_lo: 2; z = z_hi * 2 + z_lo), core: 2. Of those that a mesh axis runs over, the one named last changes fastest.
Arguments:
- ref_gate: bfloat16 [6144, 11008], P('fsdp', 'tp'), may hold values from -6 to 6
- ref_up: bfloat16 [6144, 11008], P('fsdp', 'tp'), may hold values from -6 to 6
- ref_residual: bfloat16 [6144, 4096], P('fsdp', 'tp'), may hold values from -6 to 6
- ref_modality: int32 [6144], P('fsdp'), may hold values 0 or 1
- ref_down_text: bfloat16 [4096, 11008], P('fsdp', 'tp'), may hold values from -0.0546875 to 0.0546875
- ref_down_image: bfloat16 [4096, 11008], P('fsdp', 'tp'), may hold values from -0.0546875 to 0.0546875
- pol_gate: bfloat16 [6144, 11008], P('fsdp', 'tp'), may hold values from -6 to 6
- pol_up: bfloat16 [6144, 11008], P('fsdp', 'tp'), may hold values from -6 to 6
- pol_modality: int32 [6144], P('fsdp'), may hold values 0 or 1
- pol_segment: int32 [6144], P('fsdp'), may hold values from 0 to 11, never falling along the last dimension, each value on 1 to 768 neighbouring positions
- pair_margin: float32 [6], replicated, may hold values from -30 to 30
- token_cotangent: bfloat16 [6144, 4096], P('fsdp', 'tp'), may hold values from -24 to 24
- pol_down_text: bfloat16 [4096, 11008], P('fsdp', 'tp'), may hold values from -0.0546875 to 0.0546875
- pol_down_image: bfloat16 [4096, 11008], P('fsdp', 'tp'), may hold values from -0.0546875 to 0.0546875
Outputs:
- ref_out: bfloat16 [6144, 4096], P('fsdp', 'tp')
- grad_gate: bfloat16 [6144, 11008], P('fsdp', 'tp')
- grad_up: bfloat16 [6144, 11008], P('fsdp', 'tp')
- grad_down_text: float32 [4096, 11008], P('fsdp', 'tp')
- grad_down_image: float32 [4096, 11008], P('fsdp', 'tp')
The draws below stay inside these ranges and needn't reach their ends.
Inputs may be any that keep to these rules, and one draw needn't show every extreme that they name: `ref_modality`: 0 marks a text token, 1 an image token. `pol_modality`: 0 marks a text token, 1 an image token. `pol_segment`: response numbers never fall along the tokens; responses 2p and 2p + 1 are the chosen and the rejected response of pair p; every response has at least one token.
All inputs are finite; a program needn't handle non-finite values. No bound on the sum of `ref_modality` or of `pol_modality` on one device may be relied on, other than what follows from the above.
Results may differ from the reference program's by a relative error of at most 0.015.
Values may be sent and summed in bfloat16 or wider, within the bound.
No kernel may reach another device: no remote copies, remote signals or barrier semaphores. Data moves between devices by JAX's collectives and lax.ppermute only.
A program may use at most 128 MiB of HBM per device.

```python
import math
import jax
import jax.numpy as jnp
import numpy as np
from jax import lax

D = 4096
FF = 11008
SEQ = 512
TOKENS = 6144
PAIRS = 6
N_FSDP = 8
N_TP = 16


def plant(entries, rng, smallest, top_value):
    longest = entries.shape.index(max(entries.shape))
    spots = []
    for shift in (0, 1):
        where = [jax.random.randint(jax.random.fold_in(rng, axis), (), 0, length) for axis, length in enumerate(entries.shape)]
        where[longest] = (where[longest] + shift) % entries.shape[longest]
        spots.append(tuple(where))
    return entries.at[spots[0]].set(smallest).at[spots[1]].set(top_value)


def block_levels(own_key, dims, pieces, least, largest):
    def one(position, shards_of):
        steps = jax.random.uniform(jax.random.fold_in(jax.random.fold_in(own_key, 6), position), (shards_of,), jnp.float32, least / len(pieces), largest / len(pieces))
        return jnp.repeat(jnp.exp(steps), dims[position] // shards_of).reshape((-1,) + (1,) * (len(dims) - position - 1))

    factor_of = one(*pieces[0])
    for cut in pieces[1:]:
        factor_of = factor_of * one(*cut)
    return factor_of


def profile(number_of, total, bound, slope):
    weights = [(1 << 20) // math.isqrt(standing ** slope) + 1 for standing in range(2, number_of + 1)]
    spare, counts = total - bound - (number_of - 1), [1] * (number_of - 1)
    while spare > 0:
        movable = [i for i in range(number_of - 1) if counts[i] < bound]
        whole, left = sum([weights[i] for i in movable]), spare
        for i in movable:
            extra = min(bound - counts[i], max(1, left * weights[i] // whole), spare)
            counts[i] = counts[i] + extra
            spare = spare - extra
    return np.array([bound] + counts)


def ragged_sizes(own_key, amount, total, bound, lean):
    if amount == 2:
        one = jax.random.randint(own_key, (), max(1, total - bound), min(bound, total - 1) + 1)
        return jnp.stack([one, total - one])
    lengths = jnp.asarray(profile(amount, total, bound, lean), jnp.int32)
    twos = (amount - 1) // 2
    source_of, receiver = lengths[1:1 + 2 * twos:2], lengths[2:2 + 2 * twos:2]
    margin = jnp.minimum(source_of - 1, bound - receiver)
    shifted = jax.random.randint(jax.random.fold_in(own_key, 1), (twos,), 0, 1 << 20) % (margin + 1)
    lengths = lengths.at[1:1 + 2 * twos:2].set(source_of - shifted).at[2:2 + 2 * twos:2].set(receiver + shifted)
    return lengths[jax.random.permutation(jax.random.fold_in(own_key, 2), amount)]


def normal_values(rng, dims, deviation, limit, pieces=(), held_as=jnp.bfloat16):
    factor_of = block_levels(rng, dims, pieces, -0.22, 0.18) if pieces else 1.0
    result = jax.random.normal(rng, dims, jnp.float32) * deviation * factor_of
    return jnp.minimum(jnp.maximum(result, -limit), limit).astype(held_as)


def setup_inputs(seed: int = 0) -> dict:
    seeds = jax.random.split(jax.random.key(seed), 15)
    ref_gate = normal_values(seeds[0], (TOKENS, FF), 1.0, 6.0, ((0, 8), (1, 16)))
    ref_up = normal_values(seeds[1], (TOKENS, FF), 1.0, 6.0, ((0, 8), (1, 16)))
    ref_residual = normal_values(seeds[2], (TOKENS, D), 1.0, 6.0, ((0, 8), (1, 16)))
    ref_modality = plant((jax.random.randint(seeds[3], (TOKENS,), 0, 5) < 2).astype(jnp.int32), jax.random.fold_in(seeds[3], 1), 0, 1)
    ref_down_text = normal_values(seeds[4], (D, FF), FF ** -0.5, 0.0546875, ((0, 8), (1, 16)))
    ref_down_image = normal_values(seeds[5], (D, FF), FF ** -0.5, 0.0546875, ((0, 8), (1, 16)))
    pol_gate = normal_values(seeds[6], (TOKENS, FF), 1.0, 6.0, ((0, 8), (1, 16)))
    pol_up = normal_values(seeds[7], (TOKENS, FF), 1.0, 6.0, ((0, 8), (1, 16)))
    pol_modality = plant((jax.random.randint(seeds[8], (TOKENS,), 0, 5) < 2).astype(jnp.int32), jax.random.fold_in(seeds[8], 1), 0, 1)
    pol_segment = jnp.searchsorted(jnp.cumsum(ragged_sizes(seeds[9], 2 * PAIRS, TOKENS, SEQ + SEQ // 2, 0)), jnp.arange(TOKENS), side="right").astype(jnp.int32)
    pair_margin = jnp.clip(jax.random.uniform(seeds[10], (PAIRS,), jnp.float32, -30.0, 30.0), -30.0, 30.0)
    token_cotangent = normal_values(seeds[11], (TOKENS, D), 4.0, 24.0, ((0, 8), (1, 16)))
    pol_down_text = normal_values(seeds[12], (D, FF), FF ** -0.5, 0.0546875, ((0, 8), (1, 16)))
    pol_down_image = normal_values(seeds[13], (D, FF), FF ** -0.5, 0.0546875, ((0, 8), (1, 16)))
    return {"ref_gate": ref_gate, "ref_up": ref_up, "ref_residual": ref_residual, "ref_modality": ref_modality, "ref_down_text": ref_down_text, "ref_down_image": ref_down_image, "pol_gate": pol_gate, "pol_up": pol_up, "pol_modality": pol_modality, "pol_segment": pol_segment, "pair_margin": pair_margin, "token_cotangent": token_cotangent, "pol_down_text": pol_down_text, "pol_down_image": pol_down_image}


dpo_beta = 0.1


def split_hidden(gate, up, modality):
    gate_f = gate.astype(jnp.float32)
    up_f = up.astype(jnp.float32)
    sig = jax.nn.sigmoid(gate_f)
    act = gate_f * sig
    hidden = (act * up_f).astype(jnp.bfloat16)
    image = (modality == 1)[:, None]
    zero = jnp.zeros_like(hidden)
    return jnp.where(image, zero, hidden), jnp.where(image, hidden, zero), gate_f, up_f, sig, act


def reference(ref_gate, ref_up, ref_residual, ref_modality, ref_down_text, ref_down_image, pol_gate, pol_up, pol_modality, pol_segment, pair_margin, token_cotangent, pol_down_text, pol_down_image):
    ref_text, ref_image, _, _, _, _ = split_hidden(ref_gate, ref_up, ref_modality)
    block_width = FF // N_TP
    contract = (((1,), (1,)), ((), ()))

    def ref_block(index, total):
        start = (index * block_width).astype(jnp.int32)
        left_text = lax.dynamic_slice_in_dim(ref_text, start, block_width, 1)
        left_image = lax.dynamic_slice_in_dim(ref_image, start, block_width, 1)
        right_text = lax.dynamic_slice_in_dim(ref_down_text, start, block_width, 1)
        right_image = lax.dynamic_slice_in_dim(ref_down_image, start, block_width, 1)
        part = lax.dot_general(left_text, right_text, contract, preferred_element_type=jnp.float32)
        part = part + lax.dot_general(left_image, right_image, contract, preferred_element_type=jnp.float32)
        rounded = lax.optimization_barrier(part.astype(jnp.bfloat16))
        return total + rounded.astype(jnp.float32)

    summed = lax.fori_loop(0, N_TP, ref_block, jnp.zeros((TOKENS, D), jnp.float32))
    ref_out = (summed + ref_residual.astype(jnp.float32)).astype(jnp.bfloat16)

    pol_text, pol_image, gate_f, up_f, sig, act = split_hidden(pol_gate, pol_up, pol_modality)
    seg_ids = jnp.arange(2 * PAIRS, dtype=jnp.int32)
    pair_weight = dpo_beta * jax.nn.sigmoid(-dpo_beta * pair_margin)
    table = jnp.repeat(pair_weight, 2) * jnp.where(seg_ids % 2 == 0, -1.0, 1.0).astype(jnp.float32)
    coef = jnp.sum(jnp.where(pol_segment[:, None] == seg_ids[None, :], table[None, :], jnp.float32(0.0)), axis=1)
    cot = (coef[:, None] * token_cotangent.astype(jnp.float32)).astype(jnp.bfloat16)
    image_p = (pol_modality == 1)[:, None]
    zero_cot = jnp.zeros_like(cot)
    cot_text = jnp.where(image_p, zero_cot, cot)
    cot_image = jnp.where(image_p, cot, zero_cot)
    d_hidden = jnp.dot(cot_text, pol_down_text, preferred_element_type=jnp.float32)
    d_hidden = d_hidden + jnp.dot(cot_image, pol_down_image, preferred_element_type=jnp.float32)
    grad_gate = (d_hidden * up_f * sig * (1.0 + gate_f * (1.0 - sig))).astype(jnp.bfloat16)
    grad_up = (d_hidden * act).astype(jnp.bfloat16)

    rows_block = TOKENS // N_FSDP
    over_rows = (((0,), (0,)), ((), ()))

    def grad_block(index, totals):
        start = (index * rows_block).astype(jnp.int32)
        y_text = lax.dynamic_slice_in_dim(cot_text, start, rows_block, 0)
        y_image = lax.dynamic_slice_in_dim(cot_image, start, rows_block, 0)
        h_text = lax.dynamic_slice_in_dim(pol_text, start, rows_block, 0)
        h_image = lax.dynamic_slice_in_dim(pol_image, start, rows_block, 0)
        term_text = lax.dot_general(y_text, h_text, over_rows, preferred_element_type=jnp.float32)
        term_image = lax.dot_general(y_image, h_image, over_rows, preferred_element_type=jnp.float32)
        term_text = lax.optimization_barrier(term_text.astype(jnp.bfloat16)).astype(jnp.float32)
        term_image = lax.optimization_barrier(term_image.astype(jnp.bfloat16)).astype(jnp.float32)
        return (totals[0] + term_text, totals[1] + term_image)

    start_grads = (jnp.zeros((D, FF), jnp.float32), jnp.zeros((D, FF), jnp.float32))
    grad_down_text, grad_down_image = lax.fori_loop(0, N_FSDP, grad_block, start_grads)
    return (ref_out, grad_gate, grad_up, grad_down_text, grad_down_image)
```

```python
import jax
import jax.numpy as jnp
from jax import lax
from jax.experimental import pallas as pl
from jax.experimental.pallas import tpu as pltpu
from jax.sharding import PartitionSpec as P

dpo_beta = 0.1


F32 = jnp.float32
VMEM_BYTES = 63 * 2**20
BF16 = jnp.bfloat16
ANY = pl.BlockSpec(memory_space=pl.ANY)
SMEM = pl.BlockSpec(memory_space=pltpu.SMEM)
VMEM = pl.BlockSpec(memory_space=pltpu.VMEM)

NX, NY, N_FSDP, N_TP = 4, 4, 8, 16


def move_x(s):
    return [(f, (f // NX) * NX + (f % NX + s) % NX) for f in range(N_FSDP)]


def move_y(s):
    return [(k, ((k // 4 + s) % NY) * 4 + k % 4) for k in range(N_TP)]


SWAP_ZLO = [(f, f ^ NX) for f in range(N_FSDP)]
SWAP_ZHI = [(k, k ^ 2) for k in range(N_TP)]
SWAP_CORE = [(k, k ^ 1) for k in range(N_TP)]


def tile_pairs():
    pairs = []
    for f in range(N_FSDP):
        for k in range(N_TP):
            zl, xs = divmod(f, NX)
            ys, zhs, c = k // 4, (k // 2) % 2, k % 2
            x = (ys % 2) * 2 + zhs
            y = (xs - x) % NX
            zh = (ys // 2) ^ zl
            pairs.append((f * N_TP + k, (zl * NX + x) * N_TP + y * 4 + zh * 2 + c))
    return pairs


TO_GROUP = tile_pairs()
FROM_GROUP = [(b, a) for a, b in TO_GROUP]


def pad_up(n, m):
    return -(-n // m) * m


def cost(flops, nbytes):
    return pl.CostEstimate(flops=int(flops), bytes_accessed=int(nbytes), transcendentals=0)


def load_cot(me_ref, tiles, cot, sems):
    y, zh, c = me_ref[0], me_ref[1], me_ref[2]
    width = tiles[0].shape[1]
    copies = []
    for i, t in enumerate(tiles):
        r, q, h = i // 4, (i // 2) % 2, i % 2
        col = pl.multiple_of((c ^ h) * width, width)
        dst = cot.at[(y + r) % NY, zh ^ q, :, pl.ds(col, width)]
        cp = pltpu.make_async_copy(t, dst, sems.at[0])
        cp.start()
        copies.append(cp)
    return copies


def load_hidden(blocks, raw, sems):
    own, left, opp_a, opp_b, right = blocks
    split = opp_a.shape[0]
    copies = []
    for s, at, src in ((0, 0, own), (1, 0, left), (2, 0, opp_a), (2, split, opp_b), (3, 0, right)):
        cp = pltpu.make_async_copy(src, raw.at[s, pl.ds(at, src.shape[0]), :], sems.at[1 + s])
        cp.start()
        copies.append(cp)
    return copies


def dw_kernel(me_ref, mod_ref, *refs):
    tiles, halves = refs[:16], refs[16:21]
    outs = refs[21:25]
    cot, raw, acc, send, sems = refs[25:]
    waits = load_cot(me_ref, tiles, cot, sems)
    hw = load_hidden(halves, raw, sems)
    acc[...] = jnp.zeros_like(acc)
    for w in waits + hw:
        w.wait()

    def body(s, carry):
        image = mod_ref[pl.ds(s, 1), :] == 1
        h = raw[s]
        zero = jnp.zeros_like(h)
        for m in range(2):
            hm = jnp.where(image, zero, h) if m == 0 else jnp.where(image, h, zero)
            for q in range(2):
                acc[m, q] += jnp.dot(hm, cot[s, q], preferred_element_type=F32)
        return carry

    lax.fori_loop(0, NX, body, 0)
    copies = []
    for m in range(2):
        send[m] = acc[m, 1].astype(BF16)
        copies.append(pltpu.make_async_copy(acc.at[m, 0], outs[m], sems.at[5]))
        copies.append(pltpu.make_async_copy(send.at[m], outs[2 + m], sems.at[6]))
    for cp in copies:
        cp.start()
    for cp in copies:
        cp.wait()


def run_dw(me, mod, tiles, halves):
    units = halves[0].shape[0]
    tokens = halves[0].shape[1]
    rows = 2 * tiles[0].shape[1]
    return pl.pallas_call(
        dw_kernel,
        name="dw",
        out_shape=[jax.ShapeDtypeStruct((units, rows), F32)] * 2
        + [jax.ShapeDtypeStruct((units, rows), BF16)] * 2,
        in_specs=[SMEM, VMEM] + [ANY] * 21,
        out_specs=[ANY] * 4,
        scratch_shapes=[
            pltpu.VMEM((NX, 2, tokens, rows), BF16),
            pltpu.VMEM((NX, units, tokens), BF16),
            pltpu.VMEM((2, 2, units, rows), F32),
            pltpu.VMEM((2, units, rows), BF16),
            pltpu.SemaphoreType.DMA((7,)),
        ],
        cost_estimate=cost(2 * NX * tokens * rows * units * 4, 20e6),
        compiler_params=pltpu.CompilerParams(vmem_limit_bytes=VMEM_BYTES),
    )(me, mod, *tiles, *halves)


def dh_kernel(me_ref, mod_ref, *refs):
    tiles, ws = refs[:16], refs[16:20]
    outs = refs[20:28]
    cot, w, part, own, sems = refs[28:]
    waits = load_cot(me_ref, tiles, cot, sems)
    for m in range(2):
        for q in range(2):
            cp = pltpu.make_async_copy(ws[2 * q + m], w.at[m, q], sems.at[1])
            cp.start()
            waits.append(cp)
    for cp in waits:
        cp.wait()
    half = part.shape[-1]
    nt = (((1,), (1,)), ((), ()))

    def body(i, carry):
        s = (i + 2) % NX
        for j in range(2):
            both = []
            for m in range(2):
                p = None
                for q in range(2):
                    t = lax.dot_general(
                        w[m, q], cot[s, q, pl.ds(j * half, half), :], nt, preferred_element_type=F32
                    )
                    p = t if p is None else p + t
                both.append(p)
            image = mod_ref[pl.ds(s, 1), pl.ds(j * half, half)] == 1
            dh = jnp.where(image, both[1], both[0])
            part[s, j] = dh.astype(BF16)

            @pl.when(s == 0)
            def _():
                own[j] = dh

        return carry

    lax.fori_loop(0, NX, body, 0)
    copies = []
    for j in range(2):
        copies.append(pltpu.make_async_copy(own.at[j], outs[j], sems.at[2]))
        for s in range(1, NX):
            copies.append(pltpu.make_async_copy(part.at[s, j], outs[2 * s + j], sems.at[3]))
    for cp in copies:
        cp.start()
    for cp in copies:
        cp.wait()


def run_dh(me, mod, tiles, ws):
    units, rows = ws[0].shape
    tokens = tiles[0].shape[0]
    half = tokens // 2
    return pl.pallas_call(
        dh_kernel,
        name="dh",
        out_shape=[jax.ShapeDtypeStruct((units, half), F32)] * 2
        + [jax.ShapeDtypeStruct((units, half), BF16)] * 6,
        in_specs=[SMEM, VMEM] + [ANY] * 20,
        out_specs=[ANY] * 8,
        scratch_shapes=[
            pltpu.VMEM((NX, 2, tokens, rows), BF16),
            pltpu.VMEM((2, 2, units, rows), BF16),
            pltpu.VMEM((NX, 2, units, half), BF16),
            pltpu.VMEM((2, units, half), F32),
            pltpu.SemaphoreType.DMA((4,)),
        ],
        cost_estimate=cost(2 * NX * tokens * rows * units * 4, 16e6),
        compiler_params=pltpu.CompilerParams(vmem_limit_bytes=VMEM_BYTES),
    )(me, mod, *tiles, *ws)


def fwd_kernel(me_ref, mod_ref, *refs):
    halves, ws = refs[:5], refs[5:9]
    outs = refs[9:17]
    raw, wraw, wt, out, sems = refs[17:]
    y, zh, c = me_ref[0], me_ref[1], me_ref[2]
    units, padded = ws[0].shape[0], raw.shape[1]
    waits = []
    for m in range(2):
        for q in range(2):
            cp = pltpu.make_async_copy(ws[2 * q + m], wraw.at[m, q, pl.ds(0, units), :], sems.at[0])
            cp.start()
            waits.append(cp)
    waits += load_hidden(halves, raw, sems)
    if padded > units:
        raw[:, units:, :] = jnp.zeros((NX, padded - units, raw.shape[2]), BF16)
        wraw[:, :, units:, :] = jnp.zeros((2, 2, padded - units, wraw.shape[3]), BF16)
    for cp in waits:
        cp.wait()
    for m in range(2):
        for q in range(2):
            wt[m, q] = wraw[m, q].T
    block = out.shape[3]

    def body(s, carry):
        image = mod_ref[pl.ds(s, 1), :] == 1
        h = raw[s]
        zero = jnp.zeros_like(h)
        text, img = jnp.where(image, zero, h), jnp.where(image, h, zero)
        for q in range(2):
            for k in range(2):
                at = pl.ds(k * block, block)
                p = jnp.dot(wt[0, q, at, :], text, preferred_element_type=F32)
                p = p + jnp.dot(wt[1, q, at, :], img, preferred_element_type=F32)
                out[s, q, k] = p.astype(BF16)
        return carry

    lax.fori_loop(0, NX, body, 0)
    copies = []
    for r in range(NY):
        for h in range(2):
            for q in range(2):
                src = out.at[(y + r) % NY, zh ^ q, c ^ h]
                copies.append(pltpu.make_async_copy(src, outs[2 * r + h].at[q], sems.at[5]))
    for cp in copies:
        cp.start()
    for cp in copies:
        cp.wait()


def run_fwd(me, mod, halves, ws):
    units, rows = ws[0].shape
    tokens = halves[0].shape[1]
    block, padded = rows // 2, pad_up(units, 256)
    return pl.pallas_call(
        fwd_kernel,
        name="fwd",
        out_shape=[jax.ShapeDtypeStruct((2, block, tokens), BF16)] * 8,
        in_specs=[SMEM, VMEM] + [ANY] * 9,
        out_specs=[ANY] * 8,
        scratch_shapes=[
            pltpu.VMEM((NX, padded, tokens), BF16),
            pltpu.VMEM((2, 2, padded, rows), BF16),
            pltpu.VMEM((2, 2, rows, padded), BF16),
            pltpu.VMEM((NX, 2, 2, block, tokens), BF16),
            pltpu.SemaphoreType.DMA((6,)),
        ],
        cost_estimate=cost(2 * NX * tokens * rows * units * 4, 14e6),
        compiler_params=pltpu.CompilerParams(vmem_limit_bytes=VMEM_BYTES),
    )(me, mod, *halves, *ws)


def add(*terms):
    total = terms[0].astype(F32)
    for t in terms[1:]:
        total = total + t.astype(F32)
    return total.astype(BF16)


def gather_x(own):
    split = pad_up(own.shape[0] // 2, 16)
    right = lax.ppermute(own, "fsdp", move_x(1))
    left = lax.ppermute(own, "fsdp", move_x(-1))
    opp_a = lax.ppermute(right[:split], "fsdp", move_x(1))
    opp_b = lax.ppermute(left[split:], "fsdp", move_x(-1))
    return [own, left, opp_a, opp_b, right]


def hidden_of(gate_t, up_t):
    gate_f, up_f = gate_t.astype(F32), up_t.astype(F32)
    return (gate_f * jax.nn.sigmoid(gate_f) * up_f).astype(BF16)


def per_device(
    ref_gate,
    ref_up,
    ref_residual,
    ref_modality,
    ref_down_text,
    ref_down_image,
    pol_gate,
    pol_up,
    pol_modality,
    pol_segment,
    pair_margin,
    token_cotangent,
    pol_down_text,
    pol_down_image,
):
    k = lax.axis_index("tp")
    me = jnp.stack([k // 4, (k // 2) % 2, k % 2]).astype(jnp.int32)

    seg_ids = jnp.arange(2 * pair_margin.shape[0], dtype=jnp.int32)
    pair_weight = dpo_beta * jax.nn.sigmoid(-dpo_beta * pair_margin)
    table = jnp.repeat(pair_weight, 2) * jnp.where(seg_ids % 2 == 0, -1.0, 1.0).astype(F32)
    coef = jnp.sum(
        jnp.where(pol_segment[:, None] == seg_ids[None, :], table[None, :], F32(0.0)), axis=1
    )
    cot = (coef[:, None] * token_cotangent.astype(F32)).astype(BF16)
    t0 = lax.ppermute(cot, ("fsdp", "tp"), TO_GROUP)

    mods = jnp.stack([ref_modality, pol_modality])
    mod_r = lax.ppermute(mods, "fsdp", move_x(1))
    mod_l = lax.ppermute(mods, "fsdp", move_x(-1))
    mod_o = lax.ppermute(mod_r, "fsdp", move_x(1))
    mods = jnp.stack([mods, mod_l, mod_o, mod_r], axis=1)

    pol_gate_t, pol_up_t = pol_gate.T, pol_up.T
    ref_h = gather_x(hidden_of(ref_gate.T, ref_up.T))
    pol_h = gather_x(hidden_of(pol_gate_t, pol_up_t))

    def both_rows(text, image):
        own = (text.T, image.T)
        return own + tuple(lax.ppermute(w, "fsdp", SWAP_ZLO) for w in own)

    ref_w = both_rows(ref_down_text, ref_down_image)
    pol_w = both_rows(pol_down_text, pol_down_image)

    t1 = lax.ppermute(t0, "tp", SWAP_ZHI)
    r0, l0 = lax.ppermute(t0, "tp", move_y(1)), lax.ppermute(t0, "tp", move_y(-1))
    r1, l1 = lax.ppermute(t1, "tp", move_y(1)), lax.ppermute(t1, "tp", move_y(-1))
    o0, o1 = lax.ppermute(r0, "tp", move_y(1)), lax.ppermute(l1, "tp", move_y(-1))
    tiles = []
    for mine in (t0, t1, l0, l1, o0, o1, r0, r1):
        tiles += [mine, lax.ppermute(mine, "tp", SWAP_CORE)]

    parts = run_fwd(me, mods[0], ref_h, ref_w)
    summed = [add(parts[2 * r], lax.ppermute(parts[2 * r + 1], "tp", SWAP_CORE)) for r in range(NY)]
    from_l = lax.ppermute(summed[2][0], "tp", move_y(1))
    from_r = lax.ppermute(summed[2][1], "tp", move_y(-1))
    up0 = lax.ppermute(add(summed[1][0], from_l), "tp", move_y(1))
    up1 = lax.ppermute(summed[1][1], "tp", move_y(1))
    dn0 = lax.ppermute(summed[3][0], "tp", move_y(-1))
    dn1 = lax.ppermute(add(summed[3][1], from_r), "tp", move_y(-1))
    mine = add(summed[0][0], up0, dn0)
    other = add(summed[0][1], up1, dn1)
    mine = add(mine, lax.ppermute(other, "tp", SWAP_ZHI))
    mine = lax.ppermute(mine, ("fsdp", "tp"), FROM_GROUP)
    ref_out = (mine.T.astype(F32) + ref_residual.astype(F32)).astype(BF16)

    dh = run_dh(me, mods[1], tiles, pol_w)
    own_a, own_b, p1a, p1b, p2a, p2b, p3a, p3b = dh
    in_a = lax.ppermute(p2a, "fsdp", move_x(1))
    in_b = lax.ppermute(p2b, "fsdp", move_x(-1))
    r_b = lax.ppermute(p1b, "fsdp", move_x(1))
    l_a = lax.ppermute(p3a, "fsdp", move_x(-1))
    r_a = lax.ppermute(add(p1a, in_a), "fsdp", move_x(1))
    l_b = lax.ppermute(add(p3b, in_b), "fsdp", move_x(-1))
    d_a = own_a + r_a.astype(F32) + l_a.astype(F32)
    d_b = own_b + r_b.astype(F32) + l_b.astype(F32)
    d_hidden = jnp.concatenate([d_a, d_b], axis=1)
    gate_late, up_late, _ = lax.optimization_barrier((pol_gate_t, pol_up_t, own_a))
    gate_f, up_f = gate_late.astype(F32), up_late.astype(F32)
    sig = jax.nn.sigmoid(gate_f)
    grad_gate = (d_hidden * up_f * sig * (1.0 + gate_f * (1.0 - sig))).astype(BF16).T
    grad_up = (d_hidden * (gate_f * sig)).astype(BF16).T

    own_t, own_i, send_t, send_i = run_dw(me, mods[1], tiles, pol_h)
    grad_text = (own_t + lax.ppermute(send_t, "fsdp", SWAP_ZLO).astype(F32)).T
    grad_image = (own_i + lax.ppermute(send_i, "fsdp", SWAP_ZLO).astype(F32)).T
    return (ref_out, grad_gate, grad_up, grad_text, grad_image)


def solution(mesh):
    both = P("fsdp", "tp")
    rows = P("fsdp")
    in_specs = (
        both,
        both,
        both,
        rows,
        both,
        both,
        both,
        both,
        rows,
        rows,
        P(),
        both,
        both,
        both,
    )
    return jax.shard_map(
        per_device, mesh=mesh, in_specs=in_specs, out_specs=(both,) * 5, check_vma=False
    )
```
